8 devices in a mesh: rep: 2 (over z, y), nodes: 4 (over x, core).
Axes of the slice: x: 2, y: 2, z: 1, core: 2. Of those that a mesh axis runs over, the one named last changes fastest.
Arguments:
- adjacency: bfloat16 [8192, 8192], P('nodes')
- features: bfloat16 [8192, 128], P(('nodes', 'rep'))
- w_one: float32 [128, 128], replicated
- w_two: float32 [128, 40], replicated
- labels: int32 [8192], P(('nodes', 'rep'))
- label_mask: int32 [8192], P(('nodes', 'rep'))
Outputs:
- output 1: float32 [], replicated
- output 2: float32 [128, 128], replicated
- output 3: float32 [128, 40], replicated
All inputs are finite; a program needn't handle non-finite values.
Results may differ from the reference program's by a relative error of at most 0.001.
Values are sent between devices in bfloat16 or wider.
A program may use at most 1 GiB of HBM per device.

```python
import jax
import jax.numpy as jnp
from jax import lax

NUM_NODES = 8192
F_IN = 128
HIDDEN = 128
CLASSES = 40
ROW_BLOCK = 2048
NUM_BLOCKS = NUM_NODES // ROW_BLOCK


def draw_graph(graph_key):
    comm_key, act_key, edge_key = jax.random.split(graph_key, 3)
    community = jax.random.randint(comm_key, (NUM_NODES,), 0, 8)
    activity = jax.random.randint(act_key, (NUM_NODES,), 1, 5)
    node_ids = jnp.arange(NUM_NODES)

    def adj_block(block_index):
        row_start = block_index * ROW_BLOCK
        row_comm = lax.dynamic_slice(community, (row_start,), (ROW_BLOCK,))
        row_act = lax.dynamic_slice(activity, (row_start,), (ROW_BLOCK,))
        edge_draw = jax.random.randint(jax.random.fold_in(edge_key, block_index), (ROW_BLOCK, NUM_NODES), 0, 1000)
        threshold = jnp.where(row_comm[:, None] == community[None, :], 400, 60) * row_act[:, None] // 4
        self_loop = (row_start + jnp.arange(ROW_BLOCK))[:, None] == node_ids[None, :]
        edge_weight = jnp.logical_or(edge_draw < threshold, self_loop).astype(jnp.float32)
        return (edge_weight / jnp.sum(edge_weight, axis=1, keepdims=True)).astype(jnp.bfloat16)

    adjacency = lax.map(adj_block, jnp.arange(NUM_BLOCKS)).reshape(NUM_NODES, NUM_NODES)
    return adjacency, community


def draw_labels(label_key, mask_key):
    labels = jax.random.randint(label_key, (NUM_NODES,), 0, CLASSES)
    mask_draw = (jax.random.randint(mask_key, (NUM_NODES,), 0, 10) < 3).astype(jnp.int32)
    label_mask = jnp.where(jnp.arange(NUM_NODES) == 0, 1, mask_draw).astype(jnp.int32)
    return labels, label_mask


def setup_inputs(seed: int = 0) -> dict:
    root_key = jax.random.key(seed)
    graph_key, mean_key, noise_key, one_key, two_key, label_key, mask_key = jax.random.split(root_key, 7)
    adjacency, community = draw_graph(graph_key)
    comm_mean = jax.random.normal(mean_key, (8, F_IN), jnp.float32)
    feat_noise = jax.random.normal(noise_key, (NUM_NODES, F_IN), jnp.float32)
    features = (comm_mean[community] + feat_noise).astype(jnp.bfloat16)
    w_one = jax.random.normal(one_key, (F_IN, HIDDEN), jnp.float32) * F_IN ** -0.5
    w_two = jax.random.normal(two_key, (HIDDEN, CLASSES), jnp.float32) * HIDDEN ** -0.5
    labels, label_mask = draw_labels(label_key, mask_key)
    return {"adjacency": adjacency, "features": features, "w_one": w_one, "w_two": w_two, "labels": labels, "label_mask": label_mask}


def reference(adjacency, features, w_one, w_two, labels, label_mask):
    adj_blocks = adjacency.reshape(NUM_BLOCKS, ROW_BLOCK, NUM_NODES)

    def aggregate(values):
        def one_block(adj_blk):
            return jnp.dot(adj_blk, values, preferred_element_type=jnp.float32)
        return lax.map(one_block, adj_blocks).reshape(NUM_NODES, values.shape[1])

    def aggregate_t(grad_rows):
        grad_blocks = grad_rows.reshape(NUM_BLOCKS, ROW_BLOCK, grad_rows.shape[1])

        def body(acc, pair):
            adj_blk, grad_blk = pair
            contrib = lax.dot_general(adj_blk, grad_blk, (((0,), (0,)), ((), ())), preferred_element_type=jnp.float32)
            return acc + contrib, None

        init = jnp.zeros((NUM_NODES, grad_rows.shape[1]), jnp.float32)
        return lax.scan(body, init, (adj_blocks, grad_blocks))[0]

    w_one_b = w_one.astype(jnp.bfloat16)
    w_two_b = w_two.astype(jnp.bfloat16)
    y_one = jnp.dot(features, w_one_b, preferred_element_type=jnp.float32).astype(jnp.bfloat16)
    z_one = aggregate(y_one)
    h_one = jnp.maximum(z_one, 0.0).astype(jnp.bfloat16)
    y_two = jnp.dot(h_one, w_two_b, preferred_element_type=jnp.float32).astype(jnp.bfloat16)
    z_two = aggregate(y_two)
    log_probs = jax.nn.log_softmax(z_two, axis=-1)
    onehot = (labels[:, None] == jnp.arange(CLASSES)[None, :]).astype(jnp.float32)
    mask_f = label_mask.astype(jnp.float32)
    label_count = jnp.sum(mask_f)
    loss_value = -jnp.sum(mask_f * jnp.sum(onehot * log_probs, axis=-1)) / label_count
    g_two = ((jnp.exp(log_probs) - onehot) * (mask_f / label_count)[:, None]).astype(jnp.bfloat16)
    dy_two = aggregate_t(g_two).astype(jnp.bfloat16)
    dw_two = lax.dot_general(h_one, dy_two, (((0,), (0,)), ((), ())), preferred_element_type=jnp.float32)
    dh_one = jnp.dot(dy_two, w_two_b.T, preferred_element_type=jnp.float32)
    g_one = jnp.where(z_one > 0, dh_one, 0.0).astype(jnp.bfloat16)
    dy_one = aggregate_t(g_one).astype(jnp.bfloat16)
    dw_one = lax.dot_general(features, dy_one, (((0,), (0,)), ((), ())), preferred_element_type=jnp.float32)
    return (loss_value, dw_one, dw_two)
```

```python
import jax
import jax.numpy as jnp
from jax import lax
from jax.experimental import pallas as pl
from jax.experimental.pallas import tpu as pltpu
from jax.sharding import PartitionSpec as P

MESH = pl.DeviceIdType.MESH
F32, BF16 = jnp.float32, jnp.bfloat16
NB = 1024
HALF = NB // 2
HID = 128
CLS = 40
PART = 176
PHALF = PART // 2
SAME_REP = (0, 1, 4, 5)


def dot(a, b, ca=1, cb=0):
    return lax.dot_general(a, b, (((ca,), (cb,)), ((), ())), preferred_element_type=F32)


def kernel(adj, feat, w1, w2, lab, msk, o_loss, o_dw1, o_dw2,
           a_own, a_oth, xg, acc, z1t, hl, h1, yg, gg, d2, d2r, cnt, part, pr, hs, tot,
           w1v, w2v, labv, mskv,
           a_sem, in_sem, xs, xr, ys, yr, gs, gr, ds_, dr, cs, cr, ps, pr_sem):
    r = lax.axis_index("rep")
    n = lax.axis_index("nodes")
    x, c = n // 2, n % 2

    def coords(rel):
        xx = 1 - x if rel & 4 else x
        yy = 1 - r if rel & 2 else r
        cc = 1 - c if rel & 1 else c
        return yy, 2 * xx + cc

    def peer(rel):
        yy, nn = coords(rel)
        return {"rep": yy, "nodes": nn}

    def column(rel):
        yy, nn = coords(rel)
        return pl.ds(pl.multiple_of((2 * nn + yy) * NB, NB), NB)

    def remote(src, dst, ssem, rsem, rel):
        return pltpu.make_async_remote_copy(src_ref=src, dst_ref=dst, send_sem=ssem, recv_sem=rsem,
                                            device_id=peer(rel), device_id_type=MESH)

    ins = [pltpu.make_async_copy(feat, xg.at[0], in_sem.at[0]),
           pltpu.make_async_copy(w1, w1v, in_sem.at[1]),
           pltpu.make_async_copy(w2, w2v, in_sem.at[2]),
           pltpu.make_async_copy(lab, labv, in_sem.at[3]),
           pltpu.make_async_copy(msk, mskv, in_sem.at[4])]
    for cp in ins:
        cp.start()
    own_rows = pl.ds(pl.multiple_of(r * NB, NB), NB)
    oth_rows = pl.ds(pl.multiple_of((1 - r) * NB, NB), NB)
    loads = {s: pltpu.make_async_copy(adj.at[own_rows, column(s)], a_own.at[s], a_sem.at[s]) for s in range(8)}
    oth_loads = [pltpu.make_async_copy(adj.at[oth_rows, column(s)], a_oth.at[k], a_sem.at[8 + k])
                 for k, s in enumerate(SAME_REP)]

    barrier = pltpu.get_barrier_semaphore()
    for s in range(1, 8):
        pl.semaphore_signal(barrier, inc=1, device_id=peer(s), device_id_type=MESH)
    for s in (0, 1, 4, 2, 5, 3, 6, 7):
        loads[s].start()
    for cp in oth_loads:
        cp.start()
    pl.semaphore_wait(barrier, 7)

    sent = []

    def go(cp):
        cp.start()
        sent.append(cp)
        return cp

    def gather(piece, ssem, rsem, use):
        def cp(k, src, dst, half, rel):
            return go(remote(piece(src, half), piece(dst, half), ssem.at[k], rsem.at[k], rel))
        x1 = cp(0, 0, 4, 1, 4)
        y0 = cp(1, 0, 2, 0, 2)
        p = cp(2, 0, 1, None, 1)
        x0 = cp(3, 0, 4, 0, 4)
        y1 = cp(4, 0, 2, 1, 2)
        use(0, None)
        p.wait_recv()
        use(1, None)
        x1.wait_recv()
        d61 = cp(5, 4, 6, 1, 2)
        d51 = cp(6, 4, 5, 1, 1)
        y0.wait_recv()
        d60 = cp(7, 2, 6, 0, 4)
        d30 = cp(8, 2, 3, 0, 1)
        use(4, 1)
        use(2, 0)
        x0.wait_recv()
        d50 = cp(9, 4, 5, 0, 1)
        y1.wait_recv()
        d31 = cp(10, 2, 3, 1, 1)
        use(4, 0)
        use(2, 1)
        d51.wait_recv()
        d50.wait_recv()
        use(5, None)
        d30.wait_recv()
        d31.wait_recv()
        use(3, None)
        d61.wait_recv()
        d71 = cp(11, 6, 7, 1, 1)
        d60.wait_recv()
        d70 = cp(12, 6, 7, 0, 1)
        use(6, None)
        d71.wait_recv()
        d70.wait_recv()
        use(7, None)

    for cp in ins:
        cp.wait()
    b1 = w1v[...].astype(BF16)
    b2t = w2v[...].astype(BF16)
    b2 = w2v[...].T.astype(BF16)
    mask = mskv[...].astype(F32)
    cnt[0] = jnp.broadcast_to(jnp.sum(mask, axis=1, keepdims=True), (8, 128))

    def xpiece(s, half):
        return xg.at[s] if half is None else xg.at[s, pl.ds(half * HALF, HALF), :]

    waited = set()

    def xuse(s, half):
        if s not in waited:
            loads[s].wait()
            waited.add(s)
        if half is None:
            xv, av = xg[s], a_own[s]
        else:
            xv, av = xg[s, half * HALF:(half + 1) * HALF, :], a_own[s, :, half * HALF:(half + 1) * HALF]
        rhs = jnp.concatenate([xv, dot(xv, b1).astype(BF16)], axis=1)
        prod = dot(av, rhs)
        if s == 0:
            acc[...] = prod
        else:
            acc[...] += prod

    gather(xpiece, xs, xr, xuse)
    counts = [go(remote(cnt.at[0], cnt.at[s], cs.at[s - 1], cr.at[s - 1], s)) for s in range(1, 8)]

    z1 = acc[:, HID:]
    h1[...] = jnp.maximum(z1, 0.0).astype(BF16)
    yg[0] = dot(b2t, h1[...], 1, 1).astype(BF16)

    z2 = []

    def ypiece(s, half):
        return yg.at[s] if half is None else yg.at[s, :, pl.ds(half * HALF, HALF)]

    def yuse(s, half):
        if half is None:
            yv, av = yg[s], a_own[s]
        else:
            yv, av = yg[s, :, half * HALF:(half + 1) * HALF], a_own[s, :, half * HALF:(half + 1) * HALF]
        prod = dot(yv, av, 1, 1)
        z2.append(prod if not z2 else z2.pop() + prod)
        if s == 0:
            z1t[...] = acc[:, HID:].T
            ax = acc[:, :HID]
            high = ax.astype(BF16)
            hl[:, :HID] = high
            hl[:, HID:] = (ax - high.astype(F32)).astype(BF16)

    gather(ypiece, ys, yr, yuse)
    z = z2[0]

    for cp in counts:
        cp.wait_recv()
    total = cnt[0][0:1, 0:1]
    for s in range(1, 8):
        total = total + cnt[s][0:1, 0:1]
    z = z - jnp.max(z, axis=0, keepdims=True)
    logp = z - jnp.log(jnp.sum(jnp.exp(z), axis=0, keepdims=True))
    onehot = (labv[...] == lax.broadcasted_iota(jnp.int32, (CLS, NB), 0)).astype(F32)
    loss = -jnp.sum(mask * jnp.sum(onehot * logp, axis=0, keepdims=True), axis=1, keepdims=True)
    gg[0] = ((jnp.exp(logp) - onehot) * (mask / total)).astype(BF16)
    g_y = go(remote(gg.at[0], gg.at[1], gs, gr, 2))

    for cp in oth_loads:
        cp.wait()
    g_own = gg[0]
    for k, s in ((3, 5), (2, 4), (1, 1), (0, 0)):
        d2[k] = dot(g_own, a_own[s])
    g_y.wait_recv()
    g_oth = gg[1]
    d2[3] += dot(g_oth, a_oth[3])
    pair_x = go(remote(d2.at[3], d2r.at[0], ds_.at[0], dr.at[0], 1))
    d2[2] += dot(g_oth, a_oth[2])
    d2[1] += dot(g_oth, a_oth[1])
    pair_o = go(remote(d2.at[1], d2r.at[1], ds_.at[1], dr.at[1], 1))
    pair_x.wait_recv()
    d2[2] += d2r[0]
    cross = go(remote(d2.at[2], d2r.at[2], ds_.at[2], dr.at[2], 4))
    d2[0] += dot(g_oth, a_oth[0])
    pair_o.wait_recv()
    chip_sum = d2[0] + d2r[1]
    cross.wait_recv()
    d2b = (chip_sum + d2r[2]).astype(BF16)

    g1 = jnp.where(z1t[...] > 0, dot(b2, d2b), 0.0).astype(BF16)
    dw1 = dot(g1, hl[...])
    part[0:HID] = dw1[:, :HID] + dw1[:, HID:]
    part[HID:HID + CLS] = dot(d2b, h1[...])
    part[HID + CLS:] = jnp.broadcast_to(loss, (8, 128))

    mine = pl.ds(pl.multiple_of(c * PHALF, 8), PHALF)
    theirs = pl.ds(pl.multiple_of((1 - c) * PHALF, 8), PHALF)
    a1 = go(remote(part.at[theirs, :], pr, ps.at[0], pr_sem.at[0], 1))
    a1.wait_recv()
    hs[0] = part[mine, :] + pr[...]
    a2 = [go(remote(hs.at[0], hs.at[k], ps.at[k], pr_sem.at[k], rel)) for k, rel in ((3, 6), (1, 4), (2, 2))]
    for cp in a2:
        cp.wait_recv()
    tot[mine, :] = (hs[0] + hs[1]) + (hs[2] + hs[3])
    a3 = go(remote(tot.at[mine, :], tot.at[mine, :], ps.at[4], pr_sem.at[4], 1))
    a3.wait_recv()
    o_dw1[...] = tot[0:HID].T
    o_dw2[...] = tot[HID:HID + CLS]
    o_loss[...] = tot[HID + CLS:HID + CLS + 1, 0:1] / total
    for cp in sent:
        cp.wait_send()


def solution(mesh):
    any_spec = pl.BlockSpec(memory_space=pl.ANY)
    vmem_spec = pl.BlockSpec(memory_space=pltpu.VMEM)
    dma = pltpu.SemaphoreType.DMA

    call = pl.pallas_call(
        kernel,
        out_shape=(jax.ShapeDtypeStruct((1, 1), F32), jax.ShapeDtypeStruct((HID, HID), F32),
                   jax.ShapeDtypeStruct((CLS, HID), F32)),
        in_specs=[any_spec] * 6,
        out_specs=(vmem_spec,) * 3,
        scratch_shapes=[
            pltpu.VMEM((8, NB, NB), BF16),
            pltpu.VMEM((4, NB, NB), BF16),
            pltpu.VMEM((8, NB, HID), BF16),
            pltpu.VMEM((NB, 2 * HID), F32),
            pltpu.VMEM((HID, NB), F32),
            pltpu.VMEM((NB, 2 * HID), BF16),
            pltpu.VMEM((NB, HID), BF16),
            pltpu.VMEM((8, CLS, NB), BF16),
            pltpu.VMEM((2, CLS, NB), BF16),
            pltpu.VMEM((4, CLS, NB), F32),
            pltpu.VMEM((3, CLS, NB), F32),
            pltpu.VMEM((8, 8, 128), F32),
            pltpu.VMEM((PART, 128), F32),
            pltpu.VMEM((PHALF, 128), F32),
            pltpu.VMEM((4, PHALF, 128), F32),
            pltpu.VMEM((PART, 128), F32),
            pltpu.VMEM((HID, HID), F32),
            pltpu.VMEM((CLS, HID), F32),
            pltpu.VMEM((1, NB), jnp.int32),
            pltpu.VMEM((1, NB), jnp.int32),
            dma((12,)), dma((5,)), dma((13,)), dma((13,)), dma((13,)), dma((13,)),
            dma, dma, dma((3,)), dma((3,)), dma((7,)), dma((7,)), dma((5,)), dma((5,)),
        ],
        compiler_params=pltpu.CompilerParams(collective_id=0, has_side_effects=True,
                                             vmem_limit_bytes=60 * 1024 * 1024),
        name="gcn_step",
    )

    def local_step(adj_rows, features, w_one, w_two, labels, label_mask):
        loss, dw1, dw2 = call(adj_rows, features, w_one, w_two.T, labels.reshape(1, NB), label_mask.reshape(1, NB))
        return loss.reshape(()), dw1, dw2.T

    row_spec = P(("nodes", "rep"))
    return jax.shard_map(local_step, mesh=mesh,
                         in_specs=(P("nodes", None), P(("nodes", "rep"), None), P(), P(), row_spec, row_spec),
                         out_specs=(P(), P(), P()), check_vma=False)
```

```python
import jax
import jax.numpy as jnp
from jax import lax
from jax.experimental import pallas as pl
from jax.experimental.pallas import tpu as pltpu
from jax.sharding import PartitionSpec as P

MESH = pl.DeviceIdType.MESH
F32, BF16 = jnp.float32, jnp.bfloat16
NB = 1024
HALF = NB // 2
HID = 128
CLS = 40
PART = 176
PHALF = PART // 2
SAME_REP = (0, 1, 4, 5)


def dot(a, b, ca=1, cb=0):
    return lax.dot_general(a, b, (((ca,), (cb,)), ((), ())), preferred_element_type=F32)


def kernel(adj, feat, w1, w2, lab, msk, out,
           a_own, a_oth, xg, rhs, acc, z2t, z1t, hl, h1, yg, gg, d2, d2r, cnt, part, pr, hs, tot,
           w1v, w2v, labv, mskv,
           a_sem, in_sem, xs, xr, ys, yr, gs, gr, ds_, dr, cs, cr, ps, pr_sem):
    r = lax.axis_index("rep")
    n = lax.axis_index("nodes")
    x, c = n // 2, n % 2

    def coords(rel):
        xx = 1 - x if rel & 4 else x
        yy = 1 - r if rel & 2 else r
        cc = 1 - c if rel & 1 else c
        return yy, 2 * xx + cc

    def peer(rel):
        yy, nn = coords(rel)
        return {"rep": yy, "nodes": nn}

    def column(rel):
        yy, nn = coords(rel)
        return pl.ds(pl.multiple_of((2 * nn + yy) * NB, NB), NB)

    def remote(src, dst, ssem, rsem, rel):
        return pltpu.make_async_remote_copy(src_ref=src, dst_ref=dst, send_sem=ssem, recv_sem=rsem,
                                            device_id=peer(rel), device_id_type=MESH)

    ins = [pltpu.make_async_copy(feat, xg.at[0], in_sem.at[0]),
           pltpu.make_async_copy(w1, w1v, in_sem.at[1]),
           pltpu.make_async_copy(w2, w2v, in_sem.at[2]),
           pltpu.make_async_copy(lab, labv, in_sem.at[3]),
           pltpu.make_async_copy(msk, mskv, in_sem.at[4])]
    for cp in ins:
        cp.start()
    own_rows = pl.ds(pl.multiple_of(r * NB, NB), NB)
    oth_rows = pl.ds(pl.multiple_of((1 - r) * NB, NB), NB)
    loads = {s: pltpu.make_async_copy(adj.at[own_rows, column(s)], a_own.at[s], a_sem.at[s]) for s in range(8)}
    oth_loads = [pltpu.make_async_copy(adj.at[oth_rows, column(s)], a_oth.at[k], a_sem.at[8 + k])
                 for k, s in enumerate(SAME_REP)]

    barrier = pltpu.get_barrier_semaphore()
    for s in range(1, 8):
        pl.semaphore_signal(barrier, inc=1, device_id=peer(s), device_id_type=MESH)
    for s in (0, 1, 4, 2, 5, 3, 6, 7):
        loads[s].start()
    for cp in oth_loads:
        cp.start()
    pl.semaphore_wait(barrier, 7)

    sent = []

    def go(cp):
        cp.start()
        sent.append(cp)
        return cp

    def rows(ref, s, lo, hi):
        return ref.at[s, pl.ds(lo, hi - lo), :]

    def lanes(ref, s, lo, hi):
        return ref.at[s, :, pl.ds(lo, hi - lo)]

    def gather(view, ref, ssem, rsem, use, cuts, idle):
        k = iter(range(32))

        def cp(src, dst, lo, hi, rel):
            i = next(k)
            return go(remote(view(ref, src, lo, hi), view(ref, dst, lo, hi), ssem.at[i], rsem.at[i], rel))

        lo_half, hi_half = (0, HALF), (HALF, NB)
        fine = HALF // cuts
        x1 = cp(0, 4, *hi_half, 4)
        y0 = cp(0, 2, *lo_half, 2)
        p = cp(0, 1, 0, NB, 1)
        x0 = cp(0, 4, *lo_half, 4)
        y1 = cp(0, 2, *hi_half, 2)
        use([(0, 0, NB)])
        p.wait_recv()
        use([(1, 0, NB)])
        idle()
        x1.wait_recv()
        d61 = [cp(4, 6, HALF + j * fine, HALF + (j + 1) * fine, 2) for j in range(cuts)]
        d51 = cp(4, 5, *hi_half, 1)
        y0.wait_recv()
        d60 = [cp(2, 6, j * fine, (j + 1) * fine, 4) for j in range(cuts)]
        d30 = cp(2, 3, *lo_half, 1)
        use([(4, *hi_half), (2, *lo_half)])
        x0.wait_recv()
        d50 = cp(4, 5, *lo_half, 1)
        y1.wait_recv()
        d31 = cp(2, 3, *hi_half, 1)
        d51.wait_recv()
        d30.wait_recv()
        use([(4, *lo_half), (2, *hi_half), (5, *hi_half), (3, *lo_half)])
        d50.wait_recv()
        d31.wait_recv()
        use([(5, *lo_half), (3, *hi_half)])
        late = []
        for j in range(cuts):
            lo, mid = j * fine, HALF + j * fine
            d61[j].wait_recv()
            d71 = cp(6, 7, mid, mid + fine, 1)
            d60[j].wait_recv()
            d70 = cp(6, 7, lo, lo + fine, 1)
            here = [(6, mid, mid + fine), (6, lo, lo + fine)]
            if late:
                late[0].wait_recv()
                late[1].wait_recv()
                here += late[2]
            use(here)
            late = [d71, d70, [(7, mid, mid + fine), (7, lo, lo + fine)]]
        late[0].wait_recv()
        late[1].wait_recv()
        use(late[2])

    for cp in ins:
        cp.wait()
    b1 = w1v[...].astype(BF16)
    b2t = w2v[...].astype(BF16)
    b2 = w2v[...].T.astype(BF16)
    mask = mskv[...].astype(F32)
    cnt[0] = jnp.broadcast_to(jnp.sum(mask, axis=1, keepdims=True), (8, 128))

    waited = set()

    def xuse(pieces):
        first = not waited
        for s, lo, hi in pieces:
            if s not in waited:
                loads[s].wait()
            waited.add(s)
            rhs[s, lo:hi, HID:] = dot(xg[s, lo:hi, :], b1).astype(BF16)
            rhs[s, lo:hi, :HID] = xg[s, lo:hi, :]
        for m in range(0, NB, 256):
            prod = sum(dot(a_own[s, m:m + 256, lo:hi], rhs[s, lo:hi, :]) for s, lo, hi in pieces)
            if not first:
                acc[m:m + 256, :] += prod
            else:
                acc[m:m + 256, :] = prod

    gather(rows, xg, xs, xr, xuse, 2, lambda: None)
    counts = [go(remote(cnt.at[0], cnt.at[s], cs.at[s - 1], cr.at[s - 1], s)) for s in range(1, 8)]

    z1 = acc[:, HID:]
    h1[...] = jnp.maximum(z1, 0.0).astype(BF16)
    yg[0] = dot(b2t, h1[...], 1, 1).astype(BF16)

    started = []

    def yuse(pieces):
        for m in range(0, NB, HALF):
            prod = sum(dot(yg[s, :, lo:hi], a_own[s, m:m + HALF, lo:hi], 1, 1) for s, lo, hi in pieces)
            if started:
                z2t[:, m:m + HALF] += prod
            else:
                z2t[:, m:m + HALF] = prod
        started.append(1)

    def keep_for_backward():
        z1t[...] = acc[:, HID:].T
        ax = acc[:, :HID]
        high = ax.astype(BF16)
        hl[:, :HID] = high
        hl[:, HID:] = (ax - high.astype(F32)).astype(BF16)

    gather(lanes, yg, ys, yr, yuse, 1, keep_for_backward)
    z = z2t[...]

    for cp in counts:
        cp.wait_recv()
    total = cnt[0][0:1, 0:1]
    for s in range(1, 8):
        total = total + cnt[s][0:1, 0:1]
    z = z - jnp.max(z, axis=0, keepdims=True)
    logp = z - jnp.log(jnp.sum(jnp.exp(z), axis=0, keepdims=True))
    onehot = (labv[...] == lax.broadcasted_iota(jnp.int32, (CLS, NB), 0)).astype(F32)
    loss = -jnp.sum(mask * jnp.sum(onehot * logp, axis=0, keepdims=True), axis=1, keepdims=True)
    gg[0] = ((jnp.exp(logp) - onehot) * (mask / total)).astype(BF16)
    g_y = go(remote(gg.at[0], gg.at[1], gs, gr, 2))

    for cp in oth_loads:
        cp.wait()
    g_own = gg[0]
    for k, s in ((3, 5), (2, 4), (1, 1), (0, 0)):
        d2[k] = dot(g_own, a_own[s])
    g_y.wait_recv()
    g_oth = gg[1]
    halves = ((0, HALF), (HALF, NB))
    pair_x = []
    for j, (lo, hi) in enumerate(halves):
        d2[3, :, lo:hi] += dot(g_oth, a_oth[3, :, lo:hi])
        pair_x.append(go(remote(lanes(d2, 3, lo, hi), lanes(d2r, 0, lo, hi), ds_.at[j], dr.at[j], 1)))
    d2[2] += dot(g_oth, a_oth[2])
    cross = []
    for j, (lo, hi) in enumerate(halves):
        pair_x[j].wait_recv()
        d2[2, :, lo:hi] += d2r[0, :, lo:hi]
        cross.append(go(remote(lanes(d2, 2, lo, hi), lanes(d2r, 2, lo, hi), ds_.at[2 + j], dr.at[2 + j], 4)))
    d2[1] += dot(g_oth, a_oth[1])
    pair_o = go(remote(d2.at[1], d2r.at[1], ds_.at[4], dr.at[4], 1))
    d2[0] += dot(g_oth, a_oth[0])
    pair_o.wait_recv()
    d2[0] += d2r[1]
    cross[0].wait_recv()
    cross[1].wait_recv()
    d2b = (d2[0] + d2r[2]).astype(BF16)

    g1 = jnp.where(z1t[...] > 0, dot(b2, d2b), 0.0).astype(BF16)
    dw1 = dot(g1, hl[...])
    part[0:HID] = dw1[:, :HID] + dw1[:, HID:]
    part[HID:HID + CLS] = dot(d2b, h1[...])
    part[HID + CLS:] = jnp.broadcast_to(loss, (8, 128))

    mine = pl.ds(pl.multiple_of(c * PHALF, 8), PHALF)
    theirs = pl.ds(pl.multiple_of((1 - c) * PHALF, 8), PHALF)
    a1 = go(remote(part.at[theirs, :], pr, ps.at[0], pr_sem.at[0], 1))
    a1.wait_recv()
    hs[0] = part[mine, :] + pr[...]
    a2 = [go(remote(hs.at[0], hs.at[k], ps.at[k], pr_sem.at[k], rel)) for k, rel in ((3, 6), (1, 4), (2, 2))]
    for cp in a2:
        cp.wait_recv()
    tot[mine, :] = (hs[0] + hs[1]) + (hs[2] + hs[3])
    a3 = go(remote(tot.at[mine, :], tot.at[mine, :], ps.at[4], pr_sem.at[4], 1))
    a3.wait_recv()
    out[0:HID + CLS, :] = tot[0:HID + CLS, :]
    out[HID + CLS:, :] = tot[HID + CLS:, :] / total
    for cp in sent:
        cp.wait_send()


def unpack(packed, o_loss, o_dw1, o_dw2):
    o_dw1[...] = packed[0:HID].T
    o_dw2[...] = packed[HID:HID + CLS]
    o_loss[...] = packed[HID + CLS:HID + CLS + 1, 0:1]


def solution(mesh):
    any_spec = pl.BlockSpec(memory_space=pl.ANY)
    vmem_spec = pl.BlockSpec(memory_space=pltpu.VMEM)
    dma = pltpu.SemaphoreType.DMA

    call = pl.pallas_call(
        kernel,
        out_shape=jax.ShapeDtypeStruct((PART, 128), F32),
        in_specs=[any_spec] * 6,
        out_specs=vmem_spec,
        scratch_shapes=[
            pltpu.VMEM((8, NB, NB), BF16),
            pltpu.VMEM((4, NB, NB), BF16),
            pltpu.VMEM((8, NB, HID), BF16),
            pltpu.VMEM((8, NB, 2 * HID), BF16),
            pltpu.VMEM((NB, 2 * HID), F32),
            pltpu.VMEM((CLS, NB), F32),
            pltpu.VMEM((HID, NB), F32),
            pltpu.VMEM((NB, 2 * HID), BF16),
            pltpu.VMEM((NB, HID), BF16),
            pltpu.VMEM((8, CLS, NB), BF16),
            pltpu.VMEM((2, CLS, NB), BF16),
            pltpu.VMEM((4, CLS, NB), F32),
            pltpu.VMEM((3, CLS, NB), F32),
            pltpu.VMEM((8, 8, 128), F32),
            pltpu.VMEM((PART, 128), F32),
            pltpu.VMEM((PHALF, 128), F32),
            pltpu.VMEM((4, PHALF, 128), F32),
            pltpu.VMEM((PART, 128), F32),
            pltpu.VMEM((HID, HID), F32),
            pltpu.VMEM((CLS, HID), F32),
            pltpu.VMEM((1, NB), jnp.int32),
            pltpu.VMEM((1, NB), jnp.int32),
            dma((12,)), dma((5,)), dma((17,)), dma((17,)), dma((13,)), dma((13,)),
            dma, dma, dma((5,)), dma((5,)), dma((7,)), dma((7,)), dma((5,)), dma((5,)),
        ],
        compiler_params=pltpu.CompilerParams(collective_id=0, has_side_effects=True,
                                             vmem_limit_bytes=60 * 1024 * 1024),
        name="gcn_step",
    )

    unpack_call = pl.pallas_call(
        unpack,
        out_shape=(jax.ShapeDtypeStruct((1, 1), F32), jax.ShapeDtypeStruct((HID, HID), F32),
                   jax.ShapeDtypeStruct((CLS, HID), F32)),
        in_specs=[vmem_spec],
        out_specs=(vmem_spec,) * 3,
        name="unpack",
    )

    def local_step(adj_rows, features, w_one, w_two, labels, label_mask):
        packed = call(adj_rows, features, w_one, w_two.T, labels.reshape(1, NB), label_mask.reshape(1, NB))
        loss, dw1, dw2 = unpack_call(packed)
        return loss.reshape(()), dw1, dw2.T

    row_spec = P(("nodes", "rep"))
    return jax.shard_map(local_step, mesh=mesh,
                         in_specs=(P("nodes", None), P(("nodes", "rep"), None), P(), P(), row_spec, row_spec),
                         out_specs=(P(), P(), P()), check_vma=False)
```

```python
import jax
import jax.numpy as jnp
from jax import lax
from jax.experimental import pallas as pl
from jax.experimental.pallas import tpu as pltpu
from jax.sharding import PartitionSpec as P

MESH = pl.DeviceIdType.MESH
F32, BF16 = jnp.float32, jnp.bfloat16
NB = 1024
HALF = NB // 2
XP = 256
HID = 128
CLS = 40
PART = 176
PHALF = PART // 2
SAME_REP = (0, 1, 4, 5)


def dot(a, b, ca=1, cb=0):
    return lax.dot_general(a, b, (((ca,), (cb,)), ((), ())), preferred_element_type=F32)


def kernel(adj, feat, w1, w2, lab, msk, out,
           a_own, a_oth, xg, rhs, acc, z2t, z1t, hl, h1, yg, gg, d2, d2r, cnt, part, pr, hs, tot,
           w1v, w2v, labv, mskv,
           a_sem, in_sem, xs, xr, ys, yr, gs, gr, ds_, dr, cs, cr, ps, pr_sem):
    r = lax.axis_index("rep")
    n = lax.axis_index("nodes")
    x, c = n // 2, n % 2

    def coords(rel):
        xx = 1 - x if rel & 4 else x
        yy = 1 - r if rel & 2 else r
        cc = 1 - c if rel & 1 else c
        return yy, 2 * xx + cc

    def peer(rel):
        yy, nn = coords(rel)
        return {"rep": yy, "nodes": nn}

    def column(rel):
        yy, nn = coords(rel)
        return pl.ds(pl.multiple_of((2 * nn + yy) * NB, NB), NB)

    def remote(src, dst, ssem, rsem, rel):
        return pltpu.make_async_remote_copy(src_ref=src, dst_ref=dst, send_sem=ssem, recv_sem=rsem,
                                            device_id=peer(rel), device_id_type=MESH)

    ins = [pltpu.make_async_copy(feat, xg.at[0], in_sem.at[0]),
           pltpu.make_async_copy(w1, w1v, in_sem.at[1]),
           pltpu.make_async_copy(w2, w2v, in_sem.at[2]),
           pltpu.make_async_copy(lab, labv, in_sem.at[3]),
           pltpu.make_async_copy(msk, mskv, in_sem.at[4])]
    for cp in ins:
        cp.start()
    own_rows = pl.ds(pl.multiple_of(r * NB, NB), NB)
    oth_rows = pl.ds(pl.multiple_of((1 - r) * NB, NB), NB)
    loads = {s: pltpu.make_async_copy(adj.at[own_rows, column(s)], a_own.at[s], a_sem.at[s]) for s in range(8)}
    oth_loads = [pltpu.make_async_copy(adj.at[oth_rows, column(s)], a_oth.at[k], a_sem.at[8 + k])
                 for k, s in enumerate(SAME_REP)]

    barrier = pltpu.get_barrier_semaphore()
    for s in (1, 2, 4):
        pl.semaphore_signal(barrier, inc=1, device_id=peer(s), device_id_type=MESH)
    for s in (0, 1, 4, 2, 5, 3, 6, 7):
        loads[s].start()
    for cp in oth_loads:
        cp.start()
    pl.semaphore_wait(barrier, 3)

    def lanes(ref, s, lo, hi):
        return ref.at[s, :, pl.ds(lo, hi - lo)]

    sent = []

    def go(cp):
        cp.start()
        sent.append(cp)
        return cp

    def gather(view, n, ssem, rsem, use, idle):
        k = iter(range(32))

        def cp(src, dst, piece, rel):
            i = next(k)
            return go(remote(view(src, piece), view(dst, piece), ssem.at[i], rsem.at[i], rel))

        low, high = list(range(n // 2)), list(range(n // 2, n))
        xseq, yseq = high + low, low + high
        xs_, ys_ = [], []
        for j in range(n):
            xs_.append(cp(0, 4, xseq[j], 4))
            ys_.append(cp(0, 2, yseq[j], 2))
            if j == 0:
                p = cp(0, 1, None, 1)
        use([(0, i) for i in range(n)])
        p.wait_recv()
        use([(1, i) for i in range(n)])
        idle()
        held, via_y, via_x = None, [], []

        def take_held():
            held[0].wait_recv()
            held[1].wait_recv()
            return held[2]

        for j in range(n):
            xs_[j].wait_recv()
            if j < n // 2:
                via_y.append(cp(4, 6, xseq[j], 2))
            f5 = cp(4, 5, xseq[j], 1)
            ys_[j].wait_recv()
            if j < n // 2:
                via_x.append(cp(2, 6, yseq[j], 4))
            f3 = cp(2, 3, yseq[j], 1)
            use([(4, xseq[j]), (2, yseq[j])] + (take_held() if held else []))
            held = (f5, f3, [(5, xseq[j]), (3, yseq[j])])
        use(take_held())
        held = None
        for j in range(n // 2):
            via_y[j].wait_recv()
            f7y = cp(6, 7, xseq[j], 1)
            via_x[j].wait_recv()
            f7x = cp(6, 7, yseq[j], 1)
            use([(6, xseq[j]), (6, yseq[j])] + (take_held() if held else []))
            held = (f7y, f7x, [(7, xseq[j]), (7, yseq[j])])
        use(take_held())

    for cp in ins:
        cp.wait()
    b1 = w1v[...].astype(BF16)
    b2t = w2v[...].astype(BF16)
    b2 = w2v[...].T.astype(BF16)
    mask = mskv[...].astype(F32)
    cnt[0] = jnp.broadcast_to(jnp.sum(mask, axis=1, keepdims=True), (8, 128))

    waited = set()

    def xview(s, piece):
        return xg.at[s] if piece is None else xg.at[s, pl.ds(piece * XP, XP), :]

    def xuse(pieces):
        first = not waited
        parts = []
        for s, i in pieces:
            if s not in waited:
                loads[s].wait()
            waited.add(s)
            if parts and parts[-1][0] == s and parts[-1][2] == i * XP:
                parts[-1][2] += XP
            else:
                parts.append([s, i * XP, i * XP + XP])
        for s, lo, hi in parts:
            rhs[s, lo:hi, HID:] = dot(xg[s, lo:hi, :], b1).astype(BF16)
            rhs[s, lo:hi, :HID] = xg[s, lo:hi, :]
        for m in range(0, NB, 256):
            prod = sum(dot(a_own[s, m:m + 256, lo:hi], rhs[s, lo:hi, :]) for s, lo, hi in parts)
            if first:
                acc[m:m + 256, :] = prod
            else:
                acc[m:m + 256, :] += prod

    gather(xview, NB // XP, xs, xr, xuse, lambda: None)
    counts = [go(remote(cnt.at[0], cnt.at[s], cs.at[s - 1], cr.at[s - 1], s)) for s in range(1, 8)]

    z1 = acc[:, HID:]
    h1[...] = jnp.maximum(z1, 0.0).astype(BF16)
    y2 = dot(b2t, h1[...], 1, 1).astype(BF16)
    yg[0, 0] = y2[:, :HALF]
    yg[0, 1] = y2[:, HALF:]

    started = []

    def yview(s, piece):
        return yg.at[s] if piece is None else yg.at[s, piece]

    def yuse(pieces):
        for m in range(0, NB, HALF):
            prod = sum(dot(yg[s, i], a_own[s, m:m + HALF, i * HALF:(i + 1) * HALF], 1, 1) for s, i in pieces)
            if started:
                z2t[:, m:m + HALF] += prod
            else:
                z2t[:, m:m + HALF] = prod
        started.append(1)

    def keep_for_backward():
        z1t[...] = acc[:, HID:].T
        ax = acc[:, :HID]
        high = ax.astype(BF16)
        hl[:, :HID] = high
        hl[:, HID:] = (ax - high.astype(F32)).astype(BF16)

    gather(yview, 2, ys, yr, yuse, keep_for_backward)
    z = z2t[...]

    for cp in counts:
        cp.wait_recv()
    total = cnt[0][0:1, 0:1]
    for s in range(1, 8):
        total = total + cnt[s][0:1, 0:1]
    z = z - jnp.max(z, axis=0, keepdims=True)
    logp = z - jnp.log(jnp.sum(jnp.exp(z), axis=0, keepdims=True))
    onehot = (labv[...] == lax.broadcasted_iota(jnp.int32, (CLS, NB), 0)).astype(F32)
    loss = -jnp.sum(mask * jnp.sum(onehot * logp, axis=0, keepdims=True), axis=1, keepdims=True)
    g2 = ((jnp.exp(logp) - onehot) * (mask / total)).astype(BF16)
    halves = ((0, HALF), (HALF, NB))
    g_y = []
    for j, (lo, hi) in enumerate(halves):
        gg[0, j] = g2[:, lo:hi]
        g_y.append(go(remote(gg.at[0, j], gg.at[1, j], gs.at[j], gr.at[j], 2)))

    for cp in oth_loads:
        cp.wait()
    for k, s in ((3, 5), (2, 4), (1, 1), (0, 0)):
        d2[k] = sum(dot(gg[0, j], a_own[s, lo:hi, :]) for j, (lo, hi) in enumerate(halves))
    g_y[0].wait_recv()
    for k in (3, 2, 1, 0):
        d2[k] += dot(gg[1, 0], a_oth[k, 0:HALF, :])
    g_y[1].wait_recv()
    g_oth = gg[1, 1]
    pair_x = []
    for j, (lo, hi) in enumerate(halves):
        d2[3, :, lo:hi] += dot(g_oth, a_oth[3, HALF:, lo:hi])
        pair_x.append(go(remote(lanes(d2, 3, lo, hi), lanes(d2r, 0, lo, hi), ds_.at[j], dr.at[j], 1)))
    d2[2] += dot(g_oth, a_oth[2, HALF:, :])
    cross = []
    for j, (lo, hi) in enumerate(halves):
        pair_x[j].wait_recv()
        d2[2, :, lo:hi] += d2r[0, :, lo:hi]
        cross.append(go(remote(lanes(d2, 2, lo, hi), lanes(d2r, 2, lo, hi), ds_.at[2 + j], dr.at[2 + j], 4)))
    d2[1] += dot(g_oth, a_oth[1, HALF:, :])
    pair_o = go(remote(d2.at[1], d2r.at[1], ds_.at[4], dr.at[4], 1))
    d2[0] += dot(g_oth, a_oth[0, HALF:, :])
    pair_o.wait_recv()
    d2[0] += d2r[1]
    cross[0].wait_recv()
    cross[1].wait_recv()
    d2b = (d2[0] + d2r[2]).astype(BF16)

    g1 = jnp.where(z1t[...] > 0, dot(b2, d2b), 0.0).astype(BF16)
    dw1 = dot(g1, hl[...])
    part[0:HID] = dw1[:, :HID] + dw1[:, HID:]
    part[HID:HID + CLS] = dot(d2b, h1[...])
    part[HID + CLS:] = jnp.broadcast_to(loss, (8, 128))

    mine = pl.ds(pl.multiple_of(c * PHALF, 8), PHALF)
    theirs = pl.ds(pl.multiple_of((1 - c) * PHALF, 8), PHALF)
    a1 = go(remote(part.at[theirs, :], pr, ps.at[0], pr_sem.at[0], 1))
    a1.wait_recv()
    hs[0] = part[mine, :] + pr[...]
    a2 = [go(remote(hs.at[0], hs.at[k], ps.at[k], pr_sem.at[k], rel)) for k, rel in ((3, 6), (1, 4), (2, 2))]
    for cp in a2:
        cp.wait_recv()
    tot[mine, :] = (hs[0] + hs[1]) + (hs[2] + hs[3])
    a3 = go(remote(tot.at[mine, :], tot.at[mine, :], ps.at[4], pr_sem.at[4], 1))
    a3.wait_recv()
    out[0:HID + CLS, :] = tot[0:HID + CLS, :]
    out[HID + CLS:, :] = tot[HID + CLS:, :] / total
    for cp in sent:
        cp.wait_send()


def unpack(packed, o_loss, o_dw1, o_dw2):
    o_dw1[...] = packed[0:HID].T
    o_dw2[...] = packed[HID:HID + CLS]
    o_loss[...] = packed[HID + CLS:HID + CLS + 1, 0:1]


def solution(mesh):
    any_spec = pl.BlockSpec(memory_space=pl.ANY)
    vmem_spec = pl.BlockSpec(memory_space=pltpu.VMEM)
    dma = pltpu.SemaphoreType.DMA

    call = pl.pallas_call(
        kernel,
        out_shape=jax.ShapeDtypeStruct((PART, 128), F32),
        in_specs=[any_spec] * 6,
        out_specs=vmem_spec,
        scratch_shapes=[
            pltpu.VMEM((8, NB, NB), BF16),
            pltpu.VMEM((4, NB, NB), BF16),
            pltpu.VMEM((8, NB, HID), BF16),
            pltpu.VMEM((8, NB, 2 * HID), BF16),
            pltpu.VMEM((NB, 2 * HID), F32),
            pltpu.VMEM((CLS, NB), F32),
            pltpu.VMEM((HID, NB), F32),
            pltpu.VMEM((NB, 2 * HID), BF16),
            pltpu.VMEM((NB, HID), BF16),
            pltpu.VMEM((8, 2, CLS, HALF), BF16),
            pltpu.VMEM((2, 2, CLS, HALF), BF16),
            pltpu.VMEM((4, CLS, NB), F32),
            pltpu.VMEM((3, CLS, NB), F32),
            pltpu.VMEM((8, 8, 128), F32),
            pltpu.VMEM((PART, 128), F32),
            pltpu.VMEM((PHALF, 128), F32),
            pltpu.VMEM((4, PHALF, 128), F32),
            pltpu.VMEM((PART, 128), F32),
            pltpu.VMEM((HID, HID), F32),
            pltpu.VMEM((CLS, HID), F32),
            pltpu.VMEM((1, NB), jnp.int32),
            pltpu.VMEM((1, NB), jnp.int32),
            dma((12,)), dma((5,)), dma((25,)), dma((25,)), dma((13,)), dma((13,)),
            dma((2,)), dma((2,)), dma((5,)), dma((5,)), dma((7,)), dma((7,)), dma((5,)), dma((5,)),
        ],
        compiler_params=pltpu.CompilerParams(collective_id=0, has_side_effects=True,
                                             vmem_limit_bytes=40 << 20),
        name="gcn_step",
    )

    unpack_call = pl.pallas_call(
        unpack,
        out_shape=(jax.ShapeDtypeStruct((1, 1), F32), jax.ShapeDtypeStruct((HID, HID), F32),
                   jax.ShapeDtypeStruct((CLS, HID), F32)),
        in_specs=[vmem_spec],
        out_specs=(vmem_spec,) * 3,
        compiler_params=pltpu.CompilerParams(vmem_limit_bytes=4 << 20),
        name="unpack",
    )

    def local_step(adj_rows, features, w_one, w_two, labels, label_mask):
        operands = (adj_rows, features, w_one, w_two.T, labels.reshape(1, NB), label_mask.reshape(1, NB))
        packed = call(*(pltpu.with_memory_space_constraint(v, pltpu.HBM) for v in operands))
        loss, dw1, dw2 = unpack_call(packed)
        return loss.reshape(()), dw1, dw2.T

    row_spec = P(("nodes", "rep"))
    return jax.shard_map(local_step, mesh=mesh,
                         in_specs=(P("nodes", None), P(("nodes", "rep"), None), P(), P(), row_spec, row_spec),
                         out_specs=(P(), P(), P()), check_vma=False)
```

```python
import jax
import jax.numpy as jnp
from jax import lax
from jax.experimental import pallas as pl
from jax.experimental.pallas import tpu as pltpu
from jax.sharding import PartitionSpec as P

MESH = pl.DeviceIdType.MESH
F32, BF16 = jnp.float32, jnp.bfloat16
NB = 1024
HALF = NB // 2
PIECES = 4
XP = NB // PIECES
HID = 128
CLS = 40
PART = 176
PHALF = PART // 2


def dot(a, b, ca=1, cb=0):
    return lax.dot_general(a, b, (((ca,), (cb,)), ((), ())), preferred_element_type=F32)


def kernel(adj, feat, w1, w2, lab, msk, out,
           a_own, xg, rhs, acc, z2t, z1t, hl, h1, yg, gg, d2, pair, mid, last, cnt, part, pr, hs, tot,
           w1v, w2v, labv, mskv,
           a_sem, in_sem, x_sent, x_got, y_sent, y_got, d_sent, d_got, c_sent, c_got, p_sent, p_got):
    r = lax.axis_index("rep")
    n = lax.axis_index("nodes")
    x, c = n // 2, n % 2

    def coords(rel):
        xx = 1 - x if rel & 4 else x
        yy = 1 - r if rel & 2 else r
        cc = 1 - c if rel & 1 else c
        return yy, 2 * xx + cc

    def peer(rel):
        yy, nn = coords(rel)
        return {"rep": yy, "nodes": nn}

    def send(src, dst, ssem, rsem, rel):
        pltpu.make_async_remote_copy(src_ref=src, dst_ref=dst, send_sem=ssem, recv_sem=rsem,
                                     device_id=peer(rel), device_id_type=MESH).start()

    def wait(ref, sem):
        pltpu.make_async_copy(ref, ref, sem).wait()

    ins = [pltpu.make_async_copy(feat, xg.at[0], in_sem.at[0]),
           pltpu.make_async_copy(w1, w1v, in_sem.at[1]),
           pltpu.make_async_copy(w2, w2v, in_sem.at[2]),
           pltpu.make_async_copy(lab, labv, in_sem.at[3]),
           pltpu.make_async_copy(msk, mskv, in_sem.at[4])]
    for cp in ins:
        cp.start()
    barrier = pltpu.get_barrier_semaphore()
    for s in (1, 2, 4):
        pl.semaphore_signal(barrier, inc=1, device_id=peer(s), device_id_type=MESH)
    loads = {}
    own_rows = pl.ds(pl.multiple_of(r * NB, NB), NB)
    for s in (0, 1, 4, 2, 5, 3, 6, 7):
        yy, nn = coords(s)
        columns = pl.ds(pl.multiple_of((2 * nn + yy) * NB, NB), NB)
        loads[s] = pltpu.make_async_copy(adj.at[own_rows, columns], a_own.at[s], a_sem.at[s])
        loads[s].start()
    ins[0].wait()
    pl.semaphore_wait(barrier, 3)

    def gather(view, sent, got, use, group, idle):
        half = PIECES // 2
        low, high = list(range(half)), list(range(half, PIECES))
        xseq, yseq = high + low, low + high

        def cp(src, dst, piece, rel, sem):
            send(view(src, piece, piece + 1), view(dst, piece, piece + 1), sent, got.at[sem], rel)

        def two(sem):
            wait(view(0, 0, 2), got.at[sem])

        for j in range(PIECES):
            cp(0, 4, xseq[j], 4, j)
            cp(0, 2, yseq[j], 2, j)
            if j == 0:
                send(view(0, 0, PIECES), view(1, 0, PIECES), sent, got.at[4 * PIECES - 1], 1)
        use([(0, i) for i in range(PIECES)])
        wait(view(1, 0, PIECES), got.at[4 * PIECES - 1])
        use([(1, i) for i in range(PIECES)])
        idle()
        ready, held = [], []

        def across(j):
            two(2 * PIECES + j)
            cp(6, 7, xseq[j], 1, 2 * PIECES + half + j)
            cp(6, 7, yseq[j], 1, 2 * PIECES + half + j)

        for j in range(PIECES):
            two(j)
            if j < half:
                cp(4, 6, xseq[j], 2, 2 * PIECES + j)
                cp(2, 6, yseq[j], 4, 2 * PIECES + j)
            cp(4, 5, xseq[j], 1, PIECES + j)
            cp(2, 3, yseq[j], 1, PIECES + j)
            ready += [(4, xseq[j]), (2, yseq[j])]
            if j % group == group - 1:
                for i in held:
                    two(PIECES + i)
                    ready += [(5, xseq[i]), (3, yseq[i])]
                held = []
                use(ready)
                ready = []
            held.append(j)
        held = held[-group:]
        across(0)
        for i in held:
            two(PIECES + i)
            ready += [(5, xseq[i]), (3, yseq[i])]
        use(ready)
        for j in range(1, half):
            across(j)
        use([(6, i) for i in range(PIECES)])
        for j in range(half):
            two(2 * PIECES + half + j)
        use([(7, i) for i in range(PIECES)])

    def xview(s, lo, hi):
        return xg.at[s, pl.ds(lo * XP, (hi - lo) * XP), :]

    started = {}

    def xuse(pieces):
        if not started:
            for cp in ins[1:]:
                cp.wait()
            started["b1"] = w1v[...].astype(BF16)
        parts = []
        for s, i in sorted(pieces):
            if s in loads:
                loads.pop(s).wait()
            if parts and parts[-1][0] == s and parts[-1][2] == i * XP:
                parts[-1][2] += XP
            else:
                parts.append([s, i * XP, i * XP + XP])
        for s, lo, hi in parts:
            rhs[s, lo:hi, HID:] = dot(xg[s, lo:hi, :], started["b1"]).astype(BF16)
            rhs[s, lo:hi, :HID] = xg[s, lo:hi, :]
        for m in range(0, NB, 256):
            prod = sum(dot(a_own[s, m:m + 256, lo:hi], rhs[s, lo:hi, :]) for s, lo, hi in parts)
            if "x" in started:
                acc[m:m + 256, :] += prod
            else:
                acc[m:m + 256, :] = prod
        started["x"] = True

    gather(xview, x_sent, x_got, xuse, 1, lambda: None)
    b2t = w2v[...].astype(BF16)
    b2 = w2v[...].T.astype(BF16)
    mask = mskv[...].astype(F32)
    cnt[0] = jnp.broadcast_to(jnp.sum(mask, axis=1, keepdims=True), (8, 128))

    z1 = acc[:, HID:]
    h1[...] = jnp.maximum(z1, 0.0).astype(BF16)
    y2 = dot(b2t, h1[...], 1, 1).astype(BF16)
    for i in range(PIECES):
        yg[0, i] = y2[:, i * XP:(i + 1) * XP]

    def yview(s, lo, hi):
        return yg.at[s, pl.ds(lo, hi - lo)]

    def yuse(pieces):
        parts = []
        for s, i in sorted(pieces):
            if parts and parts[-1][0] == s and parts[-1][2] == i:
                parts[-1][2] += 1
            else:
                parts.append([s, i, i + 1])
        for m in range(0, NB, HALF):
            prod = sum(dot(jnp.concatenate([yg[s, i] for i in range(lo, hi)], axis=1),
                           a_own[s, m:m + HALF, lo * XP:hi * XP], 1, 1) for s, lo, hi in parts)
            if "y" in started:
                z2t[:, m:m + HALF] += prod
            else:
                z2t[:, m:m + HALF] = prod
        started["y"] = True

    def keep_for_backward():
        for s in range(1, 8):
            send(cnt.at[0], cnt.at[s], c_sent, c_got, s)
        z1t[...] = acc[:, HID:].T
        ax = acc[:, :HID]
        high = ax.astype(BF16)
        hl[:, :HID] = high
        hl[:, HID:] = (ax - high.astype(F32)).astype(BF16)

    gather(yview, y_sent, y_got, yuse, 2, keep_for_backward)

    wait(cnt.at[pl.ds(1, 7)], c_got)
    total = cnt[0][0:1, 0:1]
    for s in range(1, 8):
        total = total + cnt[s][0:1, 0:1]
    z = z2t[...]
    z = z - jnp.max(z, axis=0, keepdims=True)
    logp = z - jnp.log(jnp.sum(jnp.exp(z), axis=0, keepdims=True))
    onehot = (labv[...] == lax.broadcasted_iota(jnp.int32, (CLS, NB), 0)).astype(F32)
    loss = -jnp.sum(mask * jnp.sum(onehot * logp, axis=0, keepdims=True), axis=1, keepdims=True)
    gg[...] = ((jnp.exp(logp) - onehot) * (mask / total)).astype(BF16)

    def partial(s, q0, q1):
        prod = dot(gg[...], a_own[s, :, q0 * XP:q1 * XP])
        for q in range(q0, q1):
            d2[s, q] = prod[:, (q - q0) * XP:(q - q0 + 1) * XP]

    def to_pair(s, q0, q1, sem):
        partial(s, q0, q1)
        send(d2.at[s, pl.ds(q0, q1 - q0)], pair.at[s // 2, pl.ds(q0, q1 - q0)], d_sent, d_got.at[sem], 1)

    def from_pair(s, q0, q1, sem):
        wait(pair.at[s // 2, pl.ds(q0, q1 - q0)], d_got.at[sem])
        d2[s, q0:q1] += pair[s // 2, q0:q1]

    to_pair(7, 0, 2, 0)
    to_pair(7, 2, 4, 1)
    partial(6, 0, 4)
    from_pair(6, 0, 2, 0)
    for j in range(2):
        send(d2.at[6, j], mid.at[j], d_sent, d_got.at[5 + j], 4)
    from_pair(6, 2, 4, 1)
    for j in range(2):
        send(d2.at[6, 2 + j], mid.at[2 + j], d_sent, d_got.at[5 + j], 2)
    to_pair(5, 0, 4, 2)
    to_pair(3, 0, 4, 3)
    partial(4, 0, 4)
    from_pair(4, 0, 4, 2)
    send(d2.at[4, pl.ds(0, 2)], last.at[0, pl.ds(0, 2)], d_sent, d_got.at[7], 4)
    partial(2, 0, 4)
    from_pair(2, 0, 4, 3)
    send(d2.at[2, pl.ds(2, 2)], last.at[0, pl.ds(2, 2)], d_sent, d_got.at[7], 2)
    to_pair(1, 0, 4, 4)
    partial(0, 0, 4)
    from_pair(0, 0, 4, 4)
    for j in range(2):
        wait(mid.at[pl.ds(0, 2)], d_got.at[5 + j])
        d2[2, j] += mid[j]
        send(d2.at[2, j], last.at[1, j], d_sent, d_got.at[8 + j], 2)
        d2[4, 2 + j] += mid[2 + j]
        send(d2.at[4, 2 + j], last.at[1, 2 + j], d_sent, d_got.at[8 + j], 4)
    wait(last.at[0], d_got.at[7])
    d2[0] += last[0]
    for j in range(2):
        wait(mid.at[pl.ds(0, 2)], d_got.at[8 + j])
    d2b = jnp.concatenate([(d2[0, q] + last[1, q]).astype(BF16) for q in range(PIECES)], axis=1)

    g1 = jnp.where(z1t[...] > 0, dot(b2, d2b), 0.0).astype(BF16)
    dw1 = dot(g1, hl[...])
    part[0:HID] = dw1[:, :HID] + dw1[:, HID:]
    part[HID:HID + CLS] = dot(d2b, h1[...])
    part[HID + CLS:] = jnp.broadcast_to(loss, (8, 128))

    mine = pl.ds(pl.multiple_of(c * PHALF, 8), PHALF)
    theirs = pl.ds(pl.multiple_of((1 - c) * PHALF, 8), PHALF)
    send(part.at[theirs, :], pr, p_sent, p_got.at[0], 1)
    wait(pr, p_got.at[0])
    hs[0] = part[mine, :] + pr[...]
    for k, rel in ((3, 6), (1, 4), (2, 2)):
        send(hs.at[0], hs.at[k], p_sent, p_got.at[1], rel)
    wait(hs.at[pl.ds(1, 3)], p_got.at[1])
    tot[mine, :] = (hs[0] + hs[1]) + (hs[2] + hs[3])
    send(tot.at[mine, :], tot.at[mine, :], p_sent, p_got.at[2], 1)
    wait(pr, p_got.at[2])
    out[0:HID + CLS, :] = tot[0:HID + CLS, :]
    out[HID + CLS:, :] = tot[HID + CLS:, :] / total

    wait(xg.at[pl.ds(0, 7)], x_sent)
    wait(yg.at[pl.ds(0, 7)], y_sent)
    wait(cnt.at[pl.ds(0, 7)], c_sent)
    wait(d2.at[pl.ds(0, 7)], d_sent)
    wait(hs, p_sent)


def unpack(packed, o_loss, o_dw1, o_dw2):
    o_dw1[...] = packed[0:HID].T
    o_dw2[...] = packed[HID:HID + CLS]
    o_loss[...] = packed[HID + CLS:HID + CLS + 1, 0:1]


def solution(mesh):
    any_spec = pl.BlockSpec(memory_space=pl.ANY)
    vmem_spec = pl.BlockSpec(memory_space=pltpu.VMEM)
    dma = pltpu.SemaphoreType.DMA

    call = pl.pallas_call(
        kernel,
        out_shape=jax.ShapeDtypeStruct((PART, 128), F32),
        in_specs=[any_spec] * 6,
        out_specs=vmem_spec,
        scratch_shapes=[
            pltpu.VMEM((8, NB, NB), BF16),
            pltpu.VMEM((8, NB, HID), BF16),
            pltpu.VMEM((8, NB, 2 * HID), BF16),
            pltpu.VMEM((NB, 2 * HID), F32),
            pltpu.VMEM((CLS, NB), F32),
            pltpu.VMEM((HID, NB), F32),
            pltpu.VMEM((NB, 2 * HID), BF16),
            pltpu.VMEM((NB, HID), BF16),
            pltpu.VMEM((8, PIECES, CLS, XP), BF16),
            pltpu.VMEM((CLS, NB), BF16),
            pltpu.VMEM((8, PIECES, CLS, XP), F32),
            pltpu.VMEM((4, PIECES, CLS, XP), F32),
            pltpu.VMEM((PIECES, CLS, XP), F32),
            pltpu.VMEM((2, PIECES, CLS, XP), F32),
            pltpu.VMEM((8, 8, 128), F32),
            pltpu.VMEM((PART, 128), F32),
            pltpu.VMEM((PHALF, 128), F32),
            pltpu.VMEM((5, PHALF, 128), F32),
            pltpu.VMEM((PART, 128), F32),
            pltpu.VMEM((HID, HID), F32),
            pltpu.VMEM((CLS, HID), F32),
            pltpu.VMEM((1, NB), jnp.int32),
            pltpu.VMEM((1, NB), jnp.int32),
            dma((8,)), dma((5,)), dma, dma((4 * PIECES,)), dma, dma((4 * PIECES,)), dma, dma((10,)),
            dma, dma, dma, dma((3,)),
        ],
        compiler_params=pltpu.CompilerParams(collective_id=0, has_side_effects=True,
                                             vmem_limit_bytes=40 << 20),
        name="gcn_step",
    )

    unpack_call = pl.pallas_call(
        unpack,
        out_shape=(jax.ShapeDtypeStruct((1, 1), F32), jax.ShapeDtypeStruct((HID, HID), F32),
                   jax.ShapeDtypeStruct((CLS, HID), F32)),
        in_specs=[vmem_spec],
        out_specs=(vmem_spec,) * 3,
        compiler_params=pltpu.CompilerParams(vmem_limit_bytes=4 << 20),
        name="unpack",
    )

    def local_step(adj_rows, features, w_one, w_two, labels, label_mask):
        operands = (adj_rows, features, w_one, w_two.T, labels.reshape(1, NB), label_mask.reshape(1, NB))
        packed = call(*(pltpu.with_memory_space_constraint(v, pltpu.HBM) for v in operands))
        loss, dw1, dw2 = unpack_call(packed)
        return loss.reshape(()), dw1, dw2.T

    row_spec = P(("nodes", "rep"))
    return jax.shard_map(local_step, mesh=mesh,
                         in_specs=(P("nodes", None), P(("nodes", "rep"), None), P(), P(), row_spec, row_spec),
                         out_specs=(P(), P(), P()), check_vma=False)
```

```python
import jax
import jax.numpy as jnp
from jax import lax
from jax.experimental import pallas as pl
from jax.experimental.pallas import tpu as pltpu
from jax.sharding import PartitionSpec as P

MESH = pl.DeviceIdType.MESH
F32, BF16 = jnp.float32, jnp.bfloat16
NB = 1024
HALF = NB // 2
PIECES = 4
XP = NB // PIECES
HID = 128
CLS = 40
PART = 176
PHALF = PART // 2


def dot(a, b, ca=1, cb=0):
    return lax.dot_general(a, b, (((ca,), (cb,)), ((), ())), preferred_element_type=F32)


def kernel(adj, feat, w1, w2, lab, msk, out,
           a_own, xg, rhs, acc, z2t, z1t, hl, h1, yg, gg, d2, pair, mid, last, cnt, part, pr, hs, tot,
           w1v, w2v, labv, mskv,
           a_sem, in_sem, x_sent, x_got, y_sent, y_got, d_sent, d_got, c_sent, c_got, p_sent, p_got):
    r = lax.axis_index("rep")
    n = lax.axis_index("nodes")
    x, c = n // 2, n % 2

    def coords(rel):
        xx = 1 - x if rel & 4 else x
        yy = 1 - r if rel & 2 else r
        cc = 1 - c if rel & 1 else c
        return yy, 2 * xx + cc

    def peer(rel):
        yy, nn = coords(rel)
        return {"rep": yy, "nodes": nn}

    def send(src, dst, ssem, rsem, rel):
        pltpu.make_async_remote_copy(src_ref=src, dst_ref=dst, send_sem=ssem, recv_sem=rsem,
                                     device_id=peer(rel), device_id_type=MESH).start()

    def wait(ref, sem):
        pltpu.make_async_copy(ref, ref, sem).wait()

    ins = [pltpu.make_async_copy(feat, xg.at[0], in_sem.at[0]),
           pltpu.make_async_copy(w1, w1v, in_sem.at[1]),
           pltpu.make_async_copy(w2, w2v, in_sem.at[2]),
           pltpu.make_async_copy(lab, labv, in_sem.at[3]),
           pltpu.make_async_copy(msk, mskv, in_sem.at[4])]
    for cp in ins:
        cp.start()
    barrier = pltpu.get_barrier_semaphore()
    for s in (1, 2, 4):
        pl.semaphore_signal(barrier, inc=1, device_id=peer(s), device_id_type=MESH)
    loads = {}
    own_rows = pl.ds(pl.multiple_of(r * NB, NB), NB)
    for s in (0, 1, 4, 2, 5, 3, 6, 7):
        yy, nn = coords(s)
        columns = pl.ds(pl.multiple_of((2 * nn + yy) * NB, NB), NB)
        loads[s] = pltpu.make_async_copy(adj.at[own_rows, columns], a_own.at[s], a_sem.at[s])
        loads[s].start()
    ins[0].wait()
    pl.semaphore_wait(barrier, 3)

    def gather(view, sent, got, use, group, idle):
        half = PIECES // 2
        low, high = list(range(half)), list(range(half, PIECES))
        xseq, yseq = high + low, low + high

        def cp(src, dst, piece, rel, sem):
            send(view(src, piece, piece + 1), view(dst, piece, piece + 1), sent, got.at[sem], rel)

        def two(sem):
            wait(view(0, 0, 2), got.at[sem])

        for j in range(PIECES):
            cp(0, 4, xseq[j], 4, j)
            cp(0, 2, yseq[j], 2, j)
            if j == 0:
                send(view(0, 0, PIECES), view(1, 0, PIECES), sent, got.at[4 * PIECES - 1], 1)
        use([(0, i) for i in range(PIECES)])
        wait(view(1, 0, PIECES), got.at[4 * PIECES - 1])
        use([(1, i) for i in range(PIECES)])
        idle()
        ready, held = [], []

        def across(j):
            two(2 * PIECES + j)
            cp(6, 7, xseq[j], 1, 2 * PIECES + half + j)
            cp(6, 7, yseq[j], 1, 2 * PIECES + half + j)

        for j in range(PIECES):
            two(j)
            if j < half:
                cp(4, 6, xseq[j], 2, 2 * PIECES + j)
                cp(2, 6, yseq[j], 4, 2 * PIECES + j)
            cp(4, 5, xseq[j], 1, PIECES + j)
            cp(2, 3, yseq[j], 1, PIECES + j)
            ready += [(4, xseq[j]), (2, yseq[j])]
            if j % group == group - 1:
                for i in held:
                    two(PIECES + i)
                    ready += [(5, xseq[i]), (3, yseq[i])]
                use(ready)
                ready, held = [], list(range(j - group + 1, j + 1))
        across(0)
        for i in held:
            two(PIECES + i)
            ready += [(5, xseq[i]), (3, yseq[i])]
        use(ready)
        for j in range(1, half):
            across(j)
        use([(6, i) for i in range(PIECES)])
        for j in range(half):
            two(2 * PIECES + half + j)
        use([(7, i) for i in range(PIECES)])

    def xview(s, lo, hi):
        return xg.at[s, pl.ds(lo * XP, (hi - lo) * XP), :]

    started = {}

    def xuse(pieces):
        if not started:
            for cp in ins[1:]:
                cp.wait()
            started["b1"] = w1v[...].astype(BF16)
        parts = []
        for s, i in sorted(pieces):
            if s in loads:
                loads.pop(s).wait()
            if parts and parts[-1][0] == s and parts[-1][2] == i * XP:
                parts[-1][2] += XP
            else:
                parts.append([s, i * XP, i * XP + XP])
        for s, lo, hi in parts:
            rhs[s, lo:hi, HID:] = dot(xg[s, lo:hi, :], started["b1"]).astype(BF16)
            rhs[s, lo:hi, :HID] = xg[s, lo:hi, :]
        for m in range(0, NB, 256):
            prod = sum(dot(a_own[s, m:m + 256, lo:hi], rhs[s, lo:hi, :]) for s, lo, hi in parts)
            if "x" in started:
                acc[m:m + 256, :] += prod
            else:
                acc[m:m + 256, :] = prod
        started["x"] = True

    gather(xview, x_sent, x_got, xuse, 1, lambda: None)
    b2t = w2v[...].astype(BF16)
    b2 = w2v[...].T.astype(BF16)
    mask = mskv[...].astype(F32)
    cnt[0] = jnp.broadcast_to(jnp.sum(mask, axis=1, keepdims=True), (8, 128))

    z1 = acc[:, HID:]
    h1[...] = jnp.maximum(z1, 0.0).astype(BF16)
    y2 = dot(b2t, h1[...], 1, 1).astype(BF16)
    for i in range(PIECES):
        yg[0, i] = y2[:, i * XP:(i + 1) * XP]

    def yview(s, lo, hi):
        return yg.at[s, pl.ds(lo, hi - lo)]

    def yuse(pieces):
        parts = []
        for s, i in sorted(pieces):
            if parts and parts[-1][0] == s and parts[-1][2] == i:
                parts[-1][2] += 1
            else:
                parts.append([s, i, i + 1])
        for m in range(0, NB, HALF):
            prod = sum(dot(jnp.concatenate([yg[s, i] for i in range(lo, hi)], axis=1),
                           a_own[s, m:m + HALF, lo * XP:hi * XP], 1, 1) for s, lo, hi in parts)
            if "y" in started:
                z2t[:, m:m + HALF] += prod
            else:
                z2t[:, m:m + HALF] = prod
        started["y"] = True

    def keep_for_backward():
        for s in range(1, 8):
            send(cnt.at[0], cnt.at[s], c_sent, c_got, s)
        z1t[...] = acc[:, HID:].T
        ax = acc[:, :HID]
        high = ax.astype(BF16)
        hl[:, :HID] = high
        hl[:, HID:] = (ax - high.astype(F32)).astype(BF16)

    gather(yview, y_sent, y_got, yuse, 2, keep_for_backward)

    wait(cnt.at[pl.ds(1, 7)], c_got)
    total = cnt[0][0:1, 0:1]
    for s in range(1, 8):
        total = total + cnt[s][0:1, 0:1]
    z = z2t[...]
    z = z - jnp.max(z, axis=0, keepdims=True)
    logp = z - jnp.log(jnp.sum(jnp.exp(z), axis=0, keepdims=True))
    onehot = (labv[...] == lax.broadcasted_iota(jnp.int32, (CLS, NB), 0)).astype(F32)
    loss = -jnp.sum(mask * jnp.sum(onehot * logp, axis=0, keepdims=True), axis=1, keepdims=True)
    gg[...] = ((jnp.exp(logp) - onehot) * (mask / total)).astype(BF16)

    def partial(s, q0, q1):
        prod = dot(gg[...], a_own[s, :, q0 * XP:q1 * XP])
        for q in range(q0, q1):
            d2[s, q] = prod[:, (q - q0) * XP:(q - q0 + 1) * XP]

    def to_pair(s, q0, q1, sem):
        partial(s, q0, q1)
        send(d2.at[s, pl.ds(q0, q1 - q0)], pair.at[s // 2, pl.ds(q0, q1 - q0)], d_sent, d_got.at[sem], 1)

    def from_pair(s, q0, q1, sem):
        wait(pair.at[s // 2, pl.ds(q0, q1 - q0)], d_got.at[sem])
        d2[s, q0:q1] += pair[s // 2, q0:q1]

    def stage_one(q):
        from_pair(6, q, q + 1, q)
        send(d2.at[6, q], mid.at[q], d_sent, d_got.at[9 + q % 2], 4 if q < 2 else 2)

    to_pair(7, 0, 1, 0)
    to_pair(7, 2, 3, 2)
    partial(6, 0, 4)
    to_pair(7, 1, 2, 1)
    stage_one(0)
    to_pair(7, 3, 4, 3)
    stage_one(2)
    to_pair(5, 0, 2, 4)
    stage_one(1)
    to_pair(3, 2, 4, 5)
    stage_one(3)
    partial(4, 0, 2)
    partial(2, 2, 4)
    from_pair(4, 0, 2, 4)
    send(d2.at[4, pl.ds(0, 2)], last.at[0, pl.ds(0, 2)], d_sent, d_got.at[11], 4)
    from_pair(2, 2, 4, 5)
    send(d2.at[2, pl.ds(2, 2)], last.at[0, pl.ds(2, 2)], d_sent, d_got.at[11], 2)
    to_pair(5, 2, 4, 6)
    to_pair(3, 0, 2, 7)
    partial(4, 2, 4)
    partial(2, 0, 2)
    to_pair(1, 0, 4, 8)
    from_pair(4, 2, 4, 6)
    from_pair(2, 0, 2, 7)
    for j in range(2):
        wait(mid.at[pl.ds(0, 2)], d_got.at[9 + j])
        d2[2, j] += mid[j]
        send(d2.at[2, j], last.at[1, j], d_sent, d_got.at[12 + j], 2)
        d2[4, 2 + j] += mid[2 + j]
        send(d2.at[4, 2 + j], last.at[1, 2 + j], d_sent, d_got.at[12 + j], 4)
        if j == 0:
            partial(0, 0, 4)
    from_pair(0, 0, 4, 8)
    wait(last.at[0], d_got.at[11])
    d2[0] += last[0]
    for j in range(2):
        wait(mid.at[pl.ds(0, 2)], d_got.at[12 + j])
    d2b = jnp.concatenate([(d2[0, q] + last[1, q]).astype(BF16) for q in range(PIECES)], axis=1)

    g1 = jnp.where(z1t[...] > 0, dot(b2, d2b), 0.0).astype(BF16)
    dw1 = dot(g1, hl[...])
    part[0:HID] = dw1[:, :HID] + dw1[:, HID:]
    part[HID:HID + CLS] = dot(d2b, h1[...])
    part[HID + CLS:] = jnp.broadcast_to(loss, (8, 128))

    mine = pl.ds(pl.multiple_of(c * PHALF, 8), PHALF)
    theirs = pl.ds(pl.multiple_of((1 - c) * PHALF, 8), PHALF)
    send(part.at[theirs, :], pr, p_sent, p_got.at[0], 1)
    wait(pr, p_got.at[0])
    hs[0] = part[mine, :] + pr[...]
    for k, rel in ((3, 6), (1, 4), (2, 2)):
        send(hs.at[0], hs.at[k], p_sent, p_got.at[1], rel)
    wait(hs.at[pl.ds(1, 3)], p_got.at[1])
    tot[mine, :] = (hs[0] + hs[1]) + (hs[2] + hs[3])
    send(tot.at[mine, :], tot.at[mine, :], p_sent, p_got.at[2], 1)
    wait(pr, p_got.at[2])
    out[0:HID + CLS, :] = tot[0:HID + CLS, :]
    out[HID + CLS:, :] = tot[HID + CLS:, :] / total

    wait(xg.at[pl.ds(0, 7)], x_sent)
    wait(yg.at[pl.ds(0, 7)], y_sent)
    wait(cnt.at[pl.ds(0, 7)], c_sent)
    wait(d2.at[pl.ds(0, 7)], d_sent)
    wait(hs, p_sent)


def unpack(packed, o_loss, o_dw1, o_dw2):
    o_dw1[...] = packed[0:HID].T
    o_dw2[...] = packed[HID:HID + CLS]
    o_loss[...] = packed[HID + CLS:HID + CLS + 1, 0:1]


def solution(mesh):
    any_spec = pl.BlockSpec(memory_space=pl.ANY)
    vmem_spec = pl.BlockSpec(memory_space=pltpu.VMEM)
    dma = pltpu.SemaphoreType.DMA

    call = pl.pallas_call(
        kernel,
        out_shape=jax.ShapeDtypeStruct((PART, 128), F32),
        in_specs=[any_spec] * 6,
        out_specs=vmem_spec,
        scratch_shapes=[
            pltpu.VMEM((8, NB, NB), BF16),
            pltpu.VMEM((8, NB, HID), BF16),
            pltpu.VMEM((8, NB, 2 * HID), BF16),
            pltpu.VMEM((NB, 2 * HID), F32),
            pltpu.VMEM((CLS, NB), F32),
            pltpu.VMEM((HID, NB), F32),
            pltpu.VMEM((NB, 2 * HID), BF16),
            pltpu.VMEM((NB, HID), BF16),
            pltpu.VMEM((8, PIECES, CLS, XP), BF16),
            pltpu.VMEM((CLS, NB), BF16),
            pltpu.VMEM((8, PIECES, CLS, XP), F32),
            pltpu.VMEM((4, PIECES, CLS, XP), F32),
            pltpu.VMEM((PIECES, CLS, XP), F32),
            pltpu.VMEM((2, PIECES, CLS, XP), F32),
            pltpu.VMEM((8, 8, 128), F32),
            pltpu.VMEM((PART, 128), F32),
            pltpu.VMEM((PHALF, 128), F32),
            pltpu.VMEM((5, PHALF, 128), F32),
            pltpu.VMEM((PART, 128), F32),
            pltpu.VMEM((HID, HID), F32),
            pltpu.VMEM((CLS, HID), F32),
            pltpu.VMEM((1, NB), jnp.int32),
            pltpu.VMEM((1, NB), jnp.int32),
            dma((8,)), dma((5,)), dma, dma((4 * PIECES,)), dma, dma((4 * PIECES,)), dma, dma((14,)),
            dma, dma, dma, dma((3,)),
        ],
        compiler_params=pltpu.CompilerParams(collective_id=0, has_side_effects=True,
                                             vmem_limit_bytes=40 << 20),
        name="gcn_step",
    )

    unpack_call = pl.pallas_call(
        unpack,
        out_shape=(jax.ShapeDtypeStruct((1, 1), F32), jax.ShapeDtypeStruct((HID, HID), F32),
                   jax.ShapeDtypeStruct((CLS, HID), F32)),
        in_specs=[vmem_spec],
        out_specs=(vmem_spec,) * 3,
        compiler_params=pltpu.CompilerParams(vmem_limit_bytes=4 << 20),
        name="unpack",
    )

    def local_step(adj_rows, features, w_one, w_two, labels, label_mask):
        operands = (adj_rows, features, w_one, w_two.T, labels.reshape(1, NB), label_mask.reshape(1, NB))
        packed = call(*(pltpu.with_memory_space_constraint(v, pltpu.HBM) for v in operands))
        loss, dw1, dw2 = unpack_call(packed)
        return loss.reshape(()), dw1, dw2.T

    row_spec = P(("nodes", "rep"))
    return jax.shard_map(local_step, mesh=mesh,
                         in_specs=(P("nodes", None), P(("nodes", "rep"), None), P(), P(), row_spec, row_spec),
                         out_specs=(P(), P(), P()), check_vma=False)
```
